512 devices in a mesh: gx: 8 (over y, z_hi), gy: 8 (over x, core), gz: 8 (over z_lo).
Axes of the slice: x: 4, y: 4, z: 16 (z_hi: 2, z_lo: 8; z = z_hi * 8 + z_lo), core: 2. Of those that a mesh axis runs over, the one named last changes fastest.
Arguments:
- weights: bfloat16 [2, 216, 262144], P(None, None, ('gx', 'gy', 'gz')), may hold values from -6 to 6
- translate: bfloat16 [2, 2, 216, 216], replicated, may hold values from -0.3125 to 0.3125
- angles: float32 [216, 256], replicated, may hold values from -3.140625 to 3.140625
- box_ids: int32 [9, 262144], P(None, ('gx', 'gy', 'gz')), may hold values from 0 to 255
Outputs:
- transformed: bfloat16 [2, 216, 262144], P(None, None, ('gx', 'gy', 'gz'))
The draws below stay inside these ranges and needn't reach their ends.
All inputs are finite; a program needn't handle non-finite values.
Results may differ from the reference program's by a relative error of at most 0.018.
Values may be sent and summed in bfloat16 or wider, within the bound.
No kernel may reach another device: no remote copies, remote signals or barrier semaphores. Data moves between devices by JAX's collectives and lax.ppermute only.
A program may use at most 64 MiB of HBM per device.

```python
import jax
import jax.numpy as jnp
from jax import lax

K = 216
NBOX = 256
P_DEV = 512
LEVELS = 9
PTOT = 262144
N_GX = 8
N_GY = 8
N_GZ = 8


def touch_ends(array, stream_key, low, top_value):
    spot = [jax.random.randint(jax.random.fold_in(stream_key, axis), (), 0, length) for axis, length in enumerate(array.shape)]
    longest = array.shape.index(max(array.shape))
    beside = spot[:longest] + [(spot[longest] + 1) % array.shape[longest]] + spot[longest + 1:]
    return array.at[tuple(spot)].set(low).at[tuple(beside)].set(top_value)


def block_levels(key, extent, cuts, low, largest):
    def one(axis_at, parts):
        steps = jax.random.uniform(jax.random.fold_in(jax.random.fold_in(key, 6), axis_at), (parts,), jnp.float32, low / len(cuts), largest / len(cuts))
        return jnp.repeat(jnp.exp(steps), extent[axis_at] // parts).reshape((-1,) + (1,) * (len(extent) - axis_at - 1))

    loudness = one(*cuts[0])
    for cut in cuts[1:]:
        loudness = loudness * one(*cut)
    return loudness


def noise(rng, extent, scale, reach, shards=(), dtype=jnp.bfloat16):
    array = jax.random.normal(rng, extent, jnp.float32) * scale
    if len(shards) > 0:
        array = block_levels(rng, extent, shards, -0.22, 0.18) * array
    return jnp.clip(array, min=-reach, max=reach).astype(dtype)


def setup_inputs(seed: int = 0) -> dict:
    arg_keys = jax.random.split(jax.random.key(seed), 5)
    return {
        "weights": noise(arg_keys[0], (2, K, PTOT), 1.0, 6.0, ((2, 512),)),
        "translate": noise(arg_keys[1], (2, 2, K, K), (2 * K) ** -0.5, 0.3125),
        "angles": jnp.clip(jax.random.uniform(arg_keys[2], (K, NBOX), jnp.float32, -3.140625, 3.140625), -3.140625, 3.140625),
        "box_ids": touch_ends(jax.random.randint(arg_keys[3], (LEVELS, PTOT), 0, NBOX), jax.random.fold_in(arg_keys[3], 1), 0, NBOX - 1).astype(jnp.int32),
    }


def rotate(current, labels, cos_tab, sin_tab):
    cosines = jnp.take(cos_tab, labels, axis=1)
    sines = jnp.take(sin_tab, labels, axis=1)
    real_part = current[0].astype(jnp.float32)
    imag_part = current[1].astype(jnp.float32)
    return jnp.stack([cosines * real_part - sines * imag_part, sines * real_part + cosines * imag_part]).astype(jnp.bfloat16)


def reference(weights, translate, angles, box_ids):
    cos_tab = jnp.cos(angles)
    sin_tab = jnp.sin(angles)
    devices_all = N_GX * N_GY * N_GZ
    current = weights
    level_index = 0
    matrices = translate.astype(jnp.float32)
    for axis_size, stride in ((N_GX, N_GY * N_GZ), (N_GY, N_GZ), (N_GZ, 1)):
        for bit_no in range(axis_size.bit_length() - 1):
            low_size = stride * (1 << bit_no)
            rotated = rotate(current, box_ids[level_index], cos_tab, sin_tab)
            blocked = rotated.reshape(2, K, devices_all // (2 * low_size), 2, low_size, 2, P_DEV // 2).astype(jnp.float32)
            mixed = jnp.einsum('tcjk,rkacbvi->rjavbti', matrices, blocked, precision=lax.Precision.HIGHEST)
            current = mixed.reshape(2, K, -1).astype(jnp.bfloat16)
            level_index += 1
    return current
```

```python
import functools

import jax
import jax.numpy as jnp
from jax import lax
from jax.experimental import pallas as pl
from jax.experimental.pallas import tpu as pltpu
from jax.sharding import Mesh, PartitionSpec as P

K = 216
KP = 256
HALF = 256
ROWS = 256
LEVELS = 9
AXES = ("y", "zh", "x", "core", "zl")
BACK = ("y", "x", "core", "zl")
ID_LANE = K
HIGH_BITS = (6, 7, 3, 4, 5)
LOW_BITS = (5, 6, 7)
f32 = jnp.float32
bf16 = jnp.bfloat16


def dot(a, b):
    return jnp.dot(a, b, preferred_element_type=f32)


def turn(ids, state, tables):
    rows = ids.shape[0]
    boxes = lax.broadcasted_iota(jnp.int32, (rows, KP), 1).astype(f32)
    picked = dot(jnp.where(ids == boxes, 1.0, 0.0).astype(bf16), tables)
    cosines, sines = picked[:, :KP], picked[:, KP:]
    re, im = state[:, :KP], state[:, KP:]
    return cosines * re - sines * im, sines * re + cosines * im


def split(plane, block):
    parts = plane.reshape(plane.shape[0] // (2 * block), 2, block, KP)
    half = plane.shape[0] // 2
    return jnp.concatenate(
        [parts[:, 0].reshape(half, KP), parts[:, 1].reshape(half, KP)], axis=1
    ).astype(bf16)


def level(state, ids, tables, mats, bit):
    block = 1 << bit
    stacked = []
    for half in range(2):
        re, im = turn(ids[half], state[half], tables)
        stacked += [split(re, block), split(im, block)]
    mixed = dot(jnp.concatenate(stacked, axis=0), mats)
    quarter = ROWS // 2
    fresh = []
    for target in range(2):
        planes = []
        for plane in range(2):
            pieces = [
                mixed[
                    (2 * half + plane) * quarter : (2 * half + plane + 1) * quarter,
                    target * KP : (target + 1) * KP,
                ].reshape(quarter // block, 1, block, KP)
                for half in range(2)
            ]
            planes.append(jnp.concatenate(pieces, axis=1).reshape(ROWS, KP))
        fresh.append(jnp.concatenate(planes, axis=1).astype(bf16).astype(f32))
    return fresh


def butterfly(side_ref, got_ref, tab_ref, mat_ref, order_ref, out_ref):
    tables = tab_ref[...]
    mats = mat_ref[...]
    got = got_ref[...].astype(f32)
    re, im = turn(got[:, ID_LANE : ID_LANE + 1], got, tables)
    mixed = dot(jnp.concatenate([split(re, 64), split(im, 64)], axis=0), mats)
    state = [
        jnp.concatenate(
            [
                mixed[:ROWS, target * KP : (target + 1) * KP],
                mixed[ROWS:, target * KP : (target + 1) * KP],
            ],
            axis=1,
        ).astype(bf16).astype(f32)
        for target in range(2)
    ]
    labels = got[:, 128:256].reshape(4, 2, 64, 128)
    labels = jnp.where(side_ref[0] == 0, labels[:, 0], labels[:, 1]).reshape(ROWS, 128)
    first = ID_LANE - 128 + 1

    def ids(table, number):
        return [
            table[:, first + 8 * half + number - 1 : first + 8 * half + number]
            for half in range(2)
        ]

    for number, bit in enumerate(HIGH_BITS, 1):
        state = level(state, ids(labels, number), tables, mats, bit)
    order = order_ref[...]
    labels = dot(order[:ROWS], labels.astype(bf16))
    state = [dot(order[:ROWS], half.astype(bf16)) for half in state]
    for number, bit in enumerate(LOW_BITS, 6):
        state = level(state, ids(labels, number), tables, mats, bit)
    for half in range(2):
        out_ref[:, half * 512 : (half + 1) * 512] = dot(
            order[ROWS:], state[half].astype(bf16)
        ).astype(bf16)


def apply_levels(side, got, tables, mats, order):
    vmem = pl.BlockSpec(memory_space=pltpu.VMEM)
    return pl.pallas_call(
        butterfly,
        out_shape=jax.ShapeDtypeStruct((ROWS, 1024), bf16),
        in_specs=[pl.BlockSpec(memory_space=pltpu.SMEM)] + [vmem] * 4,
        out_specs=vmem,
        name="butterfly",
    )(side, got, tables, mats, order)


def row_order():
    row = jnp.arange(ROWS)
    moved = (row & 31) * 8 + (row >> 5)
    there = (moved[:, None] == row[None, :]).astype(bf16)
    return jnp.concatenate([there, there.T], axis=0)


def pack_tables(angles):
    wide = jnp.pad(jnp.stack([jnp.cos(angles), jnp.sin(angles)]), ((0, 0), (0, KP - K), (0, 0)))
    return wide.transpose(2, 0, 1).reshape(256, 2 * KP).astype(bf16)


def pack_mats(translate):
    wide = jnp.pad(translate, ((0, 0), (0, 0), (0, KP - K), (0, KP - K)))
    return wide.transpose(1, 3, 0, 2).reshape(2 * KP, 2 * KP)


def pack_columns(weights, box_ids):
    cols = weights.shape[2]
    il = cols // 2
    later = box_ids[1:]
    rows = jnp.concatenate(
        [
            box_ids[:1],
            jnp.tile(later[:, :il], (1, 2)),
            jnp.tile(later[:, il:], (1, 2)),
        ],
        axis=0,
    ).astype(bf16)
    first = jnp.concatenate([weights[0], rows, jnp.zeros((KP - K - 17, cols), bf16)], axis=0)
    second = jnp.pad(weights[1], ((0, KP - K), (0, 0)))
    return jnp.concatenate([first, second], axis=0).T


def shards(weights, translate, angles, box_ids):
    packed = pack_columns(weights, box_ids)
    packed = packed.reshape(2, 4, 64, 512).transpose(1, 0, 2, 3).reshape(512, 4, 128)
    got = lax.all_to_all(packed, AXES, 0, 0, tiled=True).reshape(512, 512)
    side = lax.axis_index("zh").reshape(1)
    out = apply_levels(side, got, pack_tables(angles), pack_mats(translate), row_order())
    back = lax.all_to_all(out.reshape(256, 8, 128), BACK, 0, 0, tiled=True)
    back = back.reshape(256, 2, 2, KP)[:, :, :, :K]
    return back.transpose(2, 3, 1, 0).reshape(2, K, 512)


def solution(mesh):
    grid = Mesh(mesh.devices.reshape(4, 2, 4, 2, 8), AXES)
    columns = P(None, None, AXES)
    return jax.shard_map(
        shards,
        mesh=grid,
        in_specs=(columns, P(), P(), P(None, AXES)),
        out_specs=columns,
        check_vma=False,
    )
```

```python
import jax
import jax.numpy as jnp
from jax import lax
from jax.experimental import pallas as pl
from jax.experimental.pallas import tpu as pltpu
from jax.sharding import Mesh, PartitionSpec as P

K = 216
KP = 256
HALF = 256
ROWS = 256
LEVELS = 9
AXES = ("y", "zh", "x", "core", "zl")
BACK = ("y", "x", "core", "zl")
ID_LANE = K + 16
HIGH_BITS = (6, 7, 3, 4, 5)
LOW_BITS = (5, 6, 7)
f32 = jnp.float32
bf16 = jnp.bfloat16


def dot(a, b):
    return jnp.dot(a, b, preferred_element_type=f32)


def turn(ids, state, tables):
    rows = ids.shape[0]
    boxes = lax.broadcasted_iota(jnp.int32, (rows, KP), 1).astype(f32)
    picked = dot(jnp.where(ids == boxes, 1.0, 0.0).astype(bf16), tables)
    cosines, sines = picked[:, :KP], picked[:, KP:]
    re, im = state[:, :KP], state[:, KP:]
    return cosines * re - sines * im, sines * re + cosines * im


def split(plane, block):
    parts = plane.reshape(plane.shape[0] // (2 * block), 2, block, KP)
    half = plane.shape[0] // 2
    return jnp.concatenate(
        [parts[:, 0].reshape(half, KP), parts[:, 1].reshape(half, KP)], axis=1
    ).astype(bf16)


def level(state, ids, tables, mats, bit):
    block = 1 << bit
    stacked = []
    for half in range(2):
        re, im = turn(ids[half], state[half], tables)
        stacked += [split(re, block), split(im, block)]
    mixed = dot(jnp.concatenate(stacked, axis=0), mats)
    quarter = ROWS // 2
    fresh = []
    for target in range(2):
        planes = []
        for plane in range(2):
            pieces = [
                mixed[
                    (2 * half + plane) * quarter : (2 * half + plane + 1) * quarter,
                    target * KP : (target + 1) * KP,
                ].reshape(quarter // block, 1, block, KP)
                for half in range(2)
            ]
            planes.append(jnp.concatenate(pieces, axis=1).reshape(ROWS, KP))
        fresh.append(jnp.concatenate(planes, axis=1).astype(bf16).astype(f32))
    return fresh


def butterfly(side_ref, got_ref, tab_ref, mat_ref, order_ref, out_ref, rows_ref):
    tables = tab_ref[...]
    mats = mat_ref[...]
    rows_ref[...] = got_ref[...].astype(f32)
    got = jnp.concatenate(
        [rows_ref[pl.ds(part, 2 * ROWS, stride=4), :] for part in range(4)], axis=1
    )
    re, im = turn(got[:, ID_LANE : ID_LANE + 1], got, tables)
    mixed = dot(jnp.concatenate([split(re, 64), split(im, 64)], axis=0), mats)
    state = [
        jnp.concatenate(
            [
                mixed[:ROWS, target * KP : (target + 1) * KP],
                mixed[ROWS:, target * KP : (target + 1) * KP],
            ],
            axis=1,
        ).astype(bf16).astype(f32)
        for target in range(2)
    ]
    labels = got[:, 128:256].reshape(4, 2, 64, 128)
    labels = jnp.where(side_ref[0] == 0, labels[:, 0], labels[:, 1]).reshape(ROWS, 128)
    first = K - 128

    def ids(table, number):
        return [
            table[:, first + 8 * half + number - 1 : first + 8 * half + number]
            for half in range(2)
        ]

    for number, bit in enumerate(HIGH_BITS, 1):
        state = level(state, ids(labels, number), tables, mats, bit)
    order = order_ref[...]
    labels = dot(order[:ROWS], labels.astype(bf16))
    state = [dot(order[:ROWS], half.astype(bf16)) for half in state]
    for number, bit in enumerate(LOW_BITS, 6):
        state = level(state, ids(labels, number), tables, mats, bit)
    for half in range(2):
        done = dot(order[ROWS:], state[half].astype(bf16))
        for part in range(4):
            rows_ref[pl.ds(4 * half + part, ROWS, stride=8), :] = done[
                :, part * 128 : (part + 1) * 128
            ]
    out_ref[...] = rows_ref[...].astype(bf16)


VMEM = pl.BlockSpec(memory_space=pltpu.VMEM)


def apply_levels(side, got, tables, mats, order):
    return pl.pallas_call(
        butterfly,
        out_shape=jax.ShapeDtypeStruct((2048, 128), bf16),
        in_specs=[pl.BlockSpec(memory_space=pltpu.SMEM)] + [VMEM] * 4,
        out_specs=VMEM,
        scratch_shapes=[pltpu.VMEM((2048, 128), f32)],
        compiler_params=pltpu.CompilerParams(vmem_limit_bytes=24 * 2**20),
        name="butterfly",
    )(side, got, tables, mats, order)


def across(a, b):
    return lax.dot_general(a, b, (((1,), (1,)), ((), ())), preferred_element_type=f32)


def pack(weights_ref, ids_ref, out_ref, rows_ref):
    cols = 2 * ROWS
    ids = ids_ref[...].astype(f32)
    low, high = ids[1:, :ROWS], ids[1:, ROWS:]
    labels = jnp.concatenate(
        [
            jnp.concatenate([low, low], axis=1),
            jnp.concatenate([high, high], axis=1),
            jnp.broadcast_to(ids[:1], (KP - K - 16, cols)),
        ],
        axis=0,
    )
    target = lax.broadcasted_iota(jnp.int32, (cols, cols), 0)
    source = lax.broadcasted_iota(jnp.int32, (cols, cols), 1)
    wanted = (target & 64) * 4 + (target >> 7) * 64 + (target & 63)
    chosen = jnp.where(source == wanted, 1.0, 0.0).astype(bf16)
    first = jnp.concatenate([weights_ref[0].astype(f32), labels], axis=0).astype(bf16)
    planes = [across(chosen, first), across(chosen, weights_ref[1])]
    rows_ref[pl.ds(0, cols, stride=4), :] = planes[0][:, :128]
    rows_ref[pl.ds(1, cols, stride=4), :] = planes[0][:, 128:]
    rows_ref[pl.ds(2, cols, stride=4), :] = planes[1][:, :128]
    rows_ref[pl.ds(3, cols, stride=4), :] = jnp.concatenate(
        [planes[1][:, 128:], jnp.zeros((cols, KP - K), f32)], axis=1
    )
    out_ref[...] = rows_ref[...].astype(bf16)


def pack_columns(weights, box_ids):
    return pl.pallas_call(
        pack,
        out_shape=jax.ShapeDtypeStruct((2048, 128), bf16),
        in_specs=[VMEM] * 2,
        out_specs=VMEM,
        scratch_shapes=[pltpu.VMEM((2048, 128), f32)],
        name="pack",
    )(weights, box_ids)


def unpack(back_ref, out_ref, rows_ref):
    rows_ref[...] = back_ref[...].astype(f32)
    here = lax.broadcasted_iota(jnp.int32, (128, 128), 0)
    there = lax.broadcasted_iota(jnp.int32, (128, 128), 1)
    same = jnp.where(here == there, 1.0, 0.0).astype(bf16)
    for plane in range(2):
        for half in range(2):
            pieces = [
                across(same, rows_ref[pl.ds(4 * half + 2 * plane + part, ROWS, stride=8), :].astype(bf16))
                for part in range(2)
            ]
            block = jnp.concatenate([pieces[0], pieces[1][: K - 128]], axis=0)
            out_ref[plane, :, half * ROWS : (half + 1) * ROWS] = block.astype(bf16)


def unpack_columns(back):
    return pl.pallas_call(
        unpack,
        out_shape=jax.ShapeDtypeStruct((2, K, 512), bf16),
        in_specs=[VMEM],
        out_specs=VMEM,
        scratch_shapes=[pltpu.VMEM((2048, 128), f32)],
        compiler_params=pltpu.CompilerParams(vmem_limit_bytes=12 * 2**20),
        name="unpack",
    )(back)


def row_order():
    row = jnp.arange(ROWS)
    moved = (row & 31) * 8 + (row >> 5)
    there = (moved[:, None] == row[None, :]).astype(bf16)
    return jnp.concatenate([there, there.T], axis=0)


def pack_tables(angles):
    wide = jnp.pad(jnp.stack([jnp.cos(angles), jnp.sin(angles)]), ((0, 0), (0, KP - K), (0, 0)))
    return wide.transpose(2, 0, 1).reshape(256, 2 * KP).astype(bf16)


def pack_mats(translate):
    wide = jnp.pad(translate, ((0, 0), (0, 0), (0, KP - K), (0, KP - K)))
    return wide.transpose(1, 3, 0, 2).reshape(2 * KP, 2 * KP)


def shards(weights, translate, angles, box_ids):
    packed = pack_columns(weights, box_ids).reshape(512, 4, 128)
    got = lax.all_to_all(packed, AXES, 0, 0, tiled=True).reshape(2048, 128)
    side = lax.axis_index("zh").reshape(1)
    out = apply_levels(side, got, pack_tables(angles), pack_mats(translate), row_order())
    back = lax.all_to_all(out.reshape(256, 8, 128), BACK, 0, 0, tiled=True)
    return unpack_columns(back.reshape(2048, 128))


def solution(mesh):
    grid = Mesh(mesh.devices.reshape(4, 2, 4, 2, 8), AXES)
    columns = P(None, None, AXES)
    return jax.shard_map(
        shards,
        mesh=grid,
        in_specs=(columns, P(), P(), P(None, AXES)),
        out_specs=columns,
        check_vma=False,
    )
```

```python
import jax
import jax.numpy as jnp
from jax import lax
from jax.experimental import pallas as pl
from jax.experimental.pallas import tpu as pltpu
from jax.sharding import Mesh, PartitionSpec as P

K = 216
KP = 256
HALF = 256
ROWS = 256
LEVELS = 9
AXES = ("y", "zh", "x", "core", "zl")
OUT = ("y", "zh", "x", "zl")
BACK = ("y", "x", "zl")
ID_LANE = K + 16
TAIL = K - 128
ROOM = 128 - TAIL
BITS = {1: 5, 2: 6, 4: 3, 5: 4, 6: 5, 7: 6, 8: 7}
f32 = jnp.float32
bf16 = jnp.bfloat16


def dot(a, b):
    return jnp.dot(a, b, preferred_element_type=f32)


def turn(ids, state, tables):
    rows = ids.shape[0]
    boxes = lax.broadcasted_iota(jnp.int32, (rows, KP), 1).astype(f32)
    picked = dot(jnp.where(ids == boxes, 1.0, 0.0).astype(bf16), tables)
    cosines, sines = picked[:, :KP], picked[:, KP:]
    re, im = state[:, :KP], state[:, KP:]
    return cosines * re - sines * im, sines * re + cosines * im


def split(plane, block):
    parts = plane.reshape(plane.shape[0] // (2 * block), 2, block, KP)
    half = plane.shape[0] // 2
    return jnp.concatenate(
        [parts[:, 0].reshape(half, KP), parts[:, 1].reshape(half, KP)], axis=1
    ).astype(bf16)


def level(state, ids, tables, mats, bit):
    block = 1 << bit
    stacked = []
    for half in range(2):
        re, im = turn(ids[half], state[half], tables)
        stacked += [split(re, block), split(im, block)]
    mixed = dot(jnp.concatenate(stacked, axis=0), mats)
    quarter = ROWS // 2
    fresh = []
    for target in range(2):
        planes = []
        for plane in range(2):
            pieces = [
                mixed[
                    (2 * half + plane) * quarter : (2 * half + plane + 1) * quarter,
                    target * KP : (target + 1) * KP,
                ].reshape(quarter // block, 1, block, KP)
                for half in range(2)
            ]
            planes.append(jnp.concatenate(pieces, axis=1).reshape(ROWS, KP))
        fresh.append(jnp.concatenate(planes, axis=1).astype(bf16).astype(f32))
    return fresh


def ids(labels, number):
    first = TAIL + number - 1
    return [labels[:, first + 8 * half : first + 8 * half + 1] for half in range(2)]


def round_to(values):
    return values.astype(bf16).astype(f32)


def opening(side_ref, got_ref, tab_ref, mat_ref, keep_ref, send_ref, label_ref, rows_ref):
    tables = tab_ref[...]
    mats = mat_ref[...]
    quarter = ROWS // 2
    rows_ref[...] = got_ref[...].astype(f32)
    stacked, labels = [], []
    for kept in range(2):
        got = jnp.concatenate(
            [rows_ref[pl.ds(4 * kept + part, ROWS, stride=8), :] for part in range(4)], axis=1
        )
        re, im = turn(got[:, ID_LANE : ID_LANE + 1], got, tables)
        stacked += [split(re, 32), split(im, 32)]
        tags = got[:, 128:256].reshape(4, 2, 32, 128)
        labels.append(jnp.where(side_ref[0] == 0, tags[:, 0], tags[:, 1]).reshape(quarter, 128))
    labels = jnp.concatenate(labels, axis=0)
    mixed = dot(jnp.concatenate(stacked, axis=0), mats)
    state = []
    for target in range(2):
        lanes = slice(target * KP, (target + 1) * KP)
        blocks = [mixed[n * quarter : (n + 1) * quarter, lanes] for n in range(4)]
        state.append(
            round_to(
                jnp.concatenate(
                    [
                        jnp.concatenate(blocks[:2], axis=1),
                        jnp.concatenate(blocks[2:], axis=1),
                    ],
                    axis=0,
                )
            )
        )
    for number in (1, 2):
        state = level(state, ids(labels, number), tables, mats, BITS[number])
    turned = [
        jnp.concatenate(turn(ids(labels, 3)[half], state[half], tables), axis=1).astype(bf16)
        for half in range(2)
    ]
    low = side_ref[1] == 0
    keep_ref[...] = jnp.where(low, turned[0], turned[1])
    send_ref[...] = jnp.where(low, turned[1], turned[0])
    label_ref[...] = labels.astype(bf16)


def tail_lanes(part):
    lane = lax.broadcasted_iota(jnp.int32, (ROWS // 2, 128), 1)
    return (lane >= part * ROOM) & (lane < (part + 1) * ROOM)


def closing(side_ref, keep_ref, got_ref, label_ref, tab_ref, mat_ref, order_ref, out_ref, rows_ref):
    tables = tab_ref[...]
    mats = mat_ref[...]
    labels = label_ref[...].astype(f32)
    flipped = jnp.concatenate([mats[KP:], mats[:KP]], axis=0)
    mixed = dot(
        jnp.concatenate(
            [
                jnp.concatenate([keep_ref[:, :KP], got_ref[:, :KP]], axis=1),
                jnp.concatenate([keep_ref[:, KP:], got_ref[:, KP:]], axis=1),
            ],
            axis=0,
        ),
        jnp.where(side_ref[1] == 0, mats, flipped),
    )
    state = [
        round_to(
            jnp.concatenate(
                [
                    mixed[:ROWS, target * KP : (target + 1) * KP],
                    mixed[ROWS:, target * KP : (target + 1) * KP],
                ],
                axis=1,
            )
        )
        for target in range(2)
    ]
    for number in (4, 5):
        state = level(state, ids(labels, number), tables, mats, BITS[number])
    order = order_ref[...]
    labels = dot(order[:ROWS], labels.astype(bf16))
    state = [dot(order[:ROWS], half.astype(bf16)) for half in state]
    for number in (6, 7, 8):
        state = level(state, ids(labels, number), tables, mats, BITS[number])
    quarter = ROWS // 2
    tails = []
    done = [dot(order[ROWS:], half.astype(bf16)) for half in state]
    for kept in range(2):
        for half in range(2):
            column = done[half][kept * quarter : (kept + 1) * quarter]
            for plane in range(2):
                rows_ref[pl.ds(4 * kept + 2 * half + plane, quarter, stride=14), :] = column[
                    :, plane * KP : plane * KP + 128
                ]
                tails.append(column[:, plane * KP + 128 : (plane + 1) * KP])
    for row in range(6):
        part = row % 3
        guest = jnp.where(tail_lanes(part), tails[6 + row // 3], 0.0)
        guest = pltpu.roll(guest, TAIL - part * ROOM, 1)
        rows_ref[pl.ds(8 + row, quarter, stride=14), :] = tails[row] + guest
    out_ref[...] = rows_ref[...].astype(bf16)


VMEM = pl.BlockSpec(memory_space=pltpu.VMEM)
SMEM = pl.BlockSpec(memory_space=pltpu.SMEM)
GRANT = pltpu.CompilerParams(vmem_limit_bytes=20 * 2**20)


def open_levels(side, got, tables, mats):
    half = jax.ShapeDtypeStruct((ROWS, 2 * KP), bf16)
    return pl.pallas_call(
        opening,
        out_shape=(half, half, jax.ShapeDtypeStruct((ROWS, 128), bf16)),
        in_specs=[SMEM] + [VMEM] * 3,
        out_specs=(VMEM, VMEM, VMEM),
        scratch_shapes=[pltpu.VMEM((2048, 128), f32)],
        compiler_params=GRANT,
        name="opening",
    )(side, got, tables, mats)


def close_levels(side, keep, got, labels, tables, mats, order):
    return pl.pallas_call(
        closing,
        out_shape=jax.ShapeDtypeStruct((1792, 128), bf16),
        in_specs=[SMEM] + [VMEM] * 6,
        out_specs=VMEM,
        scratch_shapes=[pltpu.VMEM((1792, 128), f32)],
        compiler_params=GRANT,
        name="closing",
    )(side, keep, got, labels, tables, mats, order)


def across(a, b):
    return lax.dot_general(a, b, (((1,), (1,)), ((), ())), preferred_element_type=f32)


def same_lane():
    here = lax.broadcasted_iota(jnp.int32, (128, 128), 0)
    there = lax.broadcasted_iota(jnp.int32, (128, 128), 1)
    return jnp.where(here == there, 1.0, 0.0).astype(bf16)


def pack(weights_ref, ids_ref, out_ref, rows_ref):
    tags = ids_ref[...].astype(f32)
    same = same_lane()
    for half in range(2):
        for kept in range(2):
            start = half * ROWS + kept * 128
            labels = jnp.concatenate(
                [
                    tags[1:, kept * 128 : (kept + 1) * 128],
                    tags[1:, ROWS + kept * 128 : ROWS + (kept + 1) * 128],
                    jnp.broadcast_to(tags[:1, start : start + 128], (KP - K - 16, 128)),
                ],
                axis=0,
            )
            first = jnp.concatenate(
                [weights_ref[0, :, start : start + 128].astype(f32), labels], axis=0
            ).astype(bf16)
            first = across(same, first)
            second = across(same, weights_ref[1, :, start : start + 128])
            pieces = [
                first[:, :128],
                first[:, 128:],
                second[:, :128],
                jnp.concatenate([second[:, 128:], jnp.zeros((128, KP - K), f32)], axis=1),
            ]
            for part, piece in enumerate(pieces):
                for y in range(4):
                    rows_ref[
                        pl.ds((2 * y + half) * 256 + 4 * kept + part, 32, stride=8), :
                    ] = piece[32 * y : 32 * (y + 1)]
    out_ref[...] = rows_ref[...].astype(bf16)


def pack_columns(weights, box_ids):
    return pl.pallas_call(
        pack,
        out_shape=jax.ShapeDtypeStruct((2048, 128), bf16),
        in_specs=[VMEM] * 2,
        out_specs=VMEM,
        scratch_shapes=[pltpu.VMEM((2048, 128), f32)],
        name="pack",
    )(weights, box_ids)


def unpack(back_ref, out_ref, rows_ref):
    rows_ref[...] = back_ref[...].astype(f32)
    same = same_lane()
    count = ROWS // 2
    shared = [rows_ref[pl.ds(8 + row, count, stride=14), :] for row in range(6)]
    tails = list(shared)
    for group in range(2):
        guest = jnp.zeros((count, 128), f32)
        for part in range(3):
            moved = pltpu.roll(shared[3 * group + part], 128 - TAIL + part * ROOM, 1)
            guest = jnp.where(tail_lanes(part), moved, guest)
        tails.append(guest)
    for kept in range(2):
        for half in range(2):
            for plane in range(2):
                number = 4 * kept + 2 * half + plane
                head = rows_ref[pl.ds(number, count, stride=14), :]
                block = jnp.concatenate(
                    [
                        across(same, head.astype(bf16)),
                        across(same, tails[number].astype(bf16))[:TAIL],
                    ],
                    axis=0,
                )
                start = half * ROWS + kept * 128
                out_ref[plane, :, start : start + 128] = block.astype(bf16)


def unpack_columns(back):
    return pl.pallas_call(
        unpack,
        out_shape=jax.ShapeDtypeStruct((2, K, 512), bf16),
        in_specs=[VMEM],
        out_specs=VMEM,
        scratch_shapes=[pltpu.VMEM((1792, 128), f32)],
        compiler_params=GRANT,
        name="unpack",
    )(back)


def row_order():
    row = jnp.arange(ROWS)
    moved = (row & 31) * 8 + (row >> 5)
    there = (moved[:, None] == row[None, :]).astype(bf16)
    return jnp.concatenate([there, there.T], axis=0)


def pack_tables(angles):
    wide = jnp.pad(jnp.stack([jnp.cos(angles), jnp.sin(angles)]), ((0, 0), (0, KP - K), (0, 0)))
    return wide.transpose(2, 0, 1).reshape(256, 2 * KP).astype(bf16)


def pack_mats(translate):
    wide = jnp.pad(translate, ((0, 0), (0, 0), (0, KP - K), (0, KP - K)))
    return wide.transpose(1, 3, 0, 2).reshape(2 * KP, 2 * KP)


def shards(weights, translate, angles, box_ids):
    packed = pack_columns(weights, box_ids).reshape(256, 8, 128)
    got = lax.all_to_all(packed, OUT, 0, 0, tiled=True).reshape(2048, 128)
    side = jnp.stack([lax.axis_index("zh"), lax.axis_index("core")])
    tables, mats = pack_tables(angles), pack_mats(translate)
    keep, send, labels = open_levels(side, got, tables, mats)
    far = lax.ppermute(send, "core", [(0, 1), (1, 0)])
    out = close_levels(side, keep, far, labels, tables, mats, row_order())
    back = lax.all_to_all(out.reshape(128, 7, 2, 128), BACK, 0, 0, tiled=True)
    return unpack_columns(back.reshape(1792, 128))


def solution(mesh):
    grid = Mesh(mesh.devices.reshape(4, 2, 4, 2, 8), AXES)
    columns = P(None, None, AXES)
    return jax.shard_map(
        shards,
        mesh=grid,
        in_specs=(columns, P(), P(), P(None, AXES)),
        out_specs=columns,
        check_vma=False,
    )
```

```python
import jax
import jax.numpy as jnp
from jax import lax
from jax.experimental import pallas as pl
from jax.experimental.pallas import tpu as pltpu
from jax.sharding import Mesh, PartitionSpec as P

K = 216
KP = 256
HALF = 256
ROWS = 256
LEVELS = 9
AXES = ("y", "zh", "x", "core", "zl")
OUT = ("zh", "zl", "y", "x")
BACK = ("zl", "y", "x")
ID_LANE = K + 16
TAIL = K - 128
ROOM = 128 - TAIL
BITS = {1: 5, 2: 6, 4: 3, 5: 4, 6: 5, 7: 6, 8: 7}
f32 = jnp.float32
bf16 = jnp.bfloat16


def dot(a, b):
    return jnp.dot(a, b, preferred_element_type=f32)


def turn(ids, state, tables):
    rows = ids.shape[0]
    boxes = lax.broadcasted_iota(jnp.int32, (rows, KP), 1).astype(f32)
    picked = dot(jnp.where(ids == boxes, 1.0, 0.0).astype(bf16), tables)
    cosines, sines = picked[:, :KP], picked[:, KP:]
    re, im = state[:, :KP], state[:, KP:]
    return cosines * re - sines * im, sines * re + cosines * im


def split(plane, block):
    parts = plane.reshape(plane.shape[0] // (2 * block), 2, block, KP)
    half = plane.shape[0] // 2
    return jnp.concatenate(
        [parts[:, 0].reshape(half, KP), parts[:, 1].reshape(half, KP)], axis=1
    ).astype(bf16)


def level(state, ids, tables, mats, bit):
    block = 1 << bit
    stacked = []
    for half in range(2):
        re, im = turn(ids[half], state[half], tables)
        stacked += [split(re, block), split(im, block)]
    mixed = dot(jnp.concatenate(stacked, axis=0), mats)
    quarter = ROWS // 2
    fresh = []
    for target in range(2):
        planes = []
        for plane in range(2):
            pieces = [
                mixed[
                    (2 * half + plane) * quarter : (2 * half + plane + 1) * quarter,
                    target * KP : (target + 1) * KP,
                ].reshape(quarter // block, 1, block, KP)
                for half in range(2)
            ]
            planes.append(jnp.concatenate(pieces, axis=1).reshape(ROWS, KP))
        fresh.append(jnp.concatenate(planes, axis=1).astype(bf16).astype(f32))
    return fresh


def ids(labels, number):
    first = TAIL + number - 1
    return [labels[:, first + 8 * half : first + 8 * half + 1] for half in range(2)]


def round_to(values):
    return values.astype(bf16).astype(f32)


def opening(side_ref, got_ref, tab_ref, mat_ref, order_ref, keep_ref, send_ref, label_ref, rows_ref):
    tables = tab_ref[...]
    mats = mat_ref[...]
    quarter = ROWS // 2
    rows_ref[...] = got_ref[...].astype(f32)
    stacked, labels = [], []
    for kept in range(2):
        got = jnp.concatenate(
            [rows_ref[pl.ds(4 * kept + part, ROWS, stride=8), :] for part in range(4)], axis=1
        )
        got = dot(order_ref[...], got.astype(bf16))
        re, im = turn(got[:, ID_LANE : ID_LANE + 1], got, tables)
        stacked += [split(re, quarter), split(im, quarter)]
        tags = got[:, 128:256]
        labels.append(jnp.where(side_ref[0] == 0, tags[:quarter], tags[quarter:]))
    labels = jnp.concatenate(labels, axis=0)
    mixed = dot(jnp.concatenate(stacked, axis=0), mats)
    state = []
    for target in range(2):
        lanes = slice(target * KP, (target + 1) * KP)
        blocks = [mixed[n * quarter : (n + 1) * quarter, lanes] for n in range(4)]
        state.append(
            round_to(
                jnp.concatenate(
                    [
                        jnp.concatenate(blocks[:2], axis=1),
                        jnp.concatenate(blocks[2:], axis=1),
                    ],
                    axis=0,
                )
            )
        )
    for number in (1, 2):
        state = level(state, ids(labels, number), tables, mats, BITS[number])
    turned = [
        jnp.concatenate(turn(ids(labels, 3)[half], state[half], tables), axis=1).astype(bf16)
        for half in range(2)
    ]
    low = side_ref[1] == 0
    keep_ref[...] = jnp.where(low, turned[0], turned[1])
    send_ref[...] = jnp.where(low, turned[1], turned[0])
    label_ref[...] = labels.astype(bf16)


def tail_lanes(part):
    lane = lax.broadcasted_iota(jnp.int32, (ROWS // 2, 128), 1)
    return (lane >= part * ROOM) & (lane < (part + 1) * ROOM)


def closing(side_ref, keep_ref, got_ref, label_ref, tab_ref, mat_ref, order_ref, out_ref, rows_ref):
    tables = tab_ref[...]
    mats = mat_ref[...]
    labels = label_ref[...].astype(f32)
    flipped = jnp.concatenate([mats[KP:], mats[:KP]], axis=0)
    mixed = dot(
        jnp.concatenate(
            [
                jnp.concatenate([keep_ref[:, :KP], got_ref[:, :KP]], axis=1),
                jnp.concatenate([keep_ref[:, KP:], got_ref[:, KP:]], axis=1),
            ],
            axis=0,
        ),
        jnp.where(side_ref[1] == 0, mats, flipped),
    )
    state = [
        round_to(
            jnp.concatenate(
                [
                    mixed[:ROWS, target * KP : (target + 1) * KP],
                    mixed[ROWS:, target * KP : (target + 1) * KP],
                ],
                axis=1,
            )
        )
        for target in range(2)
    ]
    for number in (4, 5):
        state = level(state, ids(labels, number), tables, mats, BITS[number])
    order = order_ref[...]
    labels = dot(order, labels.astype(bf16))
    state = [dot(order, half.astype(bf16)) for half in state]
    for number in (6, 7, 8):
        state = level(state, ids(labels, number), tables, mats, BITS[number])
    quarter = ROWS // 2
    tails = []
    done = [half.reshape(8, 2, 16, 2 * KP) for half in state]
    for kept in range(2):
        for half in range(2):
            column = done[half][:, kept].reshape(quarter, 2 * KP)
            for plane in range(2):
                rows_ref[pl.ds(4 * kept + 2 * half + plane, quarter, stride=14), :] = column[
                    :, plane * KP : plane * KP + 128
                ]
                tails.append(column[:, plane * KP + 128 : (plane + 1) * KP])
    for row in range(6):
        part = row % 3
        guest = jnp.where(tail_lanes(part), tails[6 + row // 3], 0.0)
        guest = pltpu.roll(guest, TAIL - part * ROOM, 1)
        rows_ref[pl.ds(8 + row, quarter, stride=14), :] = tails[row] + guest
    out_ref[...] = rows_ref[...].astype(bf16)


VMEM = pl.BlockSpec(memory_space=pltpu.VMEM)
SMEM = pl.BlockSpec(memory_space=pltpu.SMEM)
GRANT = pltpu.CompilerParams(vmem_limit_bytes=20 * 2**20)


def open_levels(side, got, tables, mats, order):
    half = jax.ShapeDtypeStruct((ROWS, 2 * KP), bf16)
    return pl.pallas_call(
        opening,
        out_shape=(half, half, jax.ShapeDtypeStruct((ROWS, 128), bf16)),
        in_specs=[SMEM] + [VMEM] * 4,
        out_specs=(VMEM, VMEM, VMEM),
        scratch_shapes=[pltpu.VMEM((2048, 128), f32)],
        compiler_params=GRANT,
        name="opening",
    )(side, got, tables, mats, order)


def close_levels(side, keep, got, labels, tables, mats, order):
    return pl.pallas_call(
        closing,
        out_shape=jax.ShapeDtypeStruct((1792, 128), bf16),
        in_specs=[SMEM] + [VMEM] * 6,
        out_specs=VMEM,
        scratch_shapes=[pltpu.VMEM((1792, 128), f32)],
        compiler_params=GRANT,
        name="closing",
    )(side, keep, got, labels, tables, mats, order)


def across(a, b):
    return lax.dot_general(a, b, (((1,), (1,)), ((), ())), preferred_element_type=f32)


def same_lane():
    here = lax.broadcasted_iota(jnp.int32, (128, 128), 0)
    there = lax.broadcasted_iota(jnp.int32, (128, 128), 1)
    return jnp.where(here == there, 1.0, 0.0).astype(bf16)


def pack(weights_ref, ids_ref, all_ids_ref, out_ref, rows_ref):
    own = ids_ref[...].astype(f32)
    tags = all_ids_ref[...].astype(f32)
    same = same_lane()
    for kept in range(2):
        lanes = slice(kept * 128, (kept + 1) * 128)
        labels = jnp.concatenate(
            [
                tags[1:, lanes],
                tags[1:, ROWS + kept * 128 : ROWS + (kept + 1) * 128],
                jnp.broadcast_to(own[:1, lanes], (KP - K - 16, 128)),
            ],
            axis=0,
        )
        first = jnp.concatenate([weights_ref[0, :, lanes].astype(f32), labels], axis=0)
        first = across(same, first.astype(bf16))
        second = across(same, weights_ref[1, :, lanes])
        pieces = [
            first[:, :128],
            first[:, 128:],
            second[:, :128],
            jnp.concatenate([second[:, 128:], jnp.zeros((128, KP - K), f32)], axis=1),
        ]
        for part, piece in enumerate(pieces):
            rows_ref[pl.ds(4 * kept + part, 128, stride=8), :] = piece
    out_ref[...] = rows_ref[...].astype(bf16)


def pack_columns(weights, box_ids):
    return pl.pallas_call(
        pack,
        grid=(2,),
        out_shape=jax.ShapeDtypeStruct((2048, 128), bf16),
        in_specs=[
            pl.BlockSpec((2, K, ROWS), lambda half: (0, 0, half)),
            pl.BlockSpec((LEVELS, ROWS), lambda half: (0, half)),
            pl.BlockSpec((LEVELS, 2 * ROWS), lambda half: (0, 0)),
        ],
        out_specs=pl.BlockSpec((1024, 128), lambda half: (half, 0)),
        scratch_shapes=[pltpu.VMEM((1024, 128), f32)],
        name="pack",
    )(weights, box_ids, box_ids)


def unpack(back_ref, out_ref, rows_ref):
    rows_ref[...] = back_ref[...].astype(f32)
    same = same_lane()
    count = ROWS // 2
    shared = [rows_ref[pl.ds(8 + row, count, stride=14), :] for row in range(6)]
    tails = list(shared)
    for group in range(2):
        guest = jnp.zeros((count, 128), f32)
        for part in range(3):
            moved = pltpu.roll(shared[3 * group + part], 128 - TAIL + part * ROOM, 1)
            guest = jnp.where(tail_lanes(part), moved, guest)
        tails.append(guest)
    for kept in range(2):
        for half in range(2):
            for plane in range(2):
                number = 4 * kept + 2 * half + plane
                head = rows_ref[pl.ds(number, count, stride=14), :]
                block = jnp.concatenate(
                    [
                        across(same, head.astype(bf16)),
                        across(same, tails[number].astype(bf16))[:TAIL],
                    ],
                    axis=0,
                )
                start = half * ROWS + kept * 128
                out_ref[plane, :, start : start + 128] = block.astype(bf16)


def unpack_columns(back):
    return pl.pallas_call(
        unpack,
        out_shape=jax.ShapeDtypeStruct((2, K, 512), bf16),
        in_specs=[VMEM],
        out_specs=VMEM,
        scratch_shapes=[pltpu.VMEM((1792, 128), f32)],
        compiler_params=GRANT,
        name="unpack",
    )(back)


def one_hot(source):
    return (source[:, None] == jnp.arange(ROWS)[None, :]).astype(bf16)


def row_orders():
    row = jnp.arange(ROWS)
    enter = one_hot((row & 128) + (row & 7) * 16 + ((row >> 3) & 15))
    return enter, one_hot((row & 31) * 8 + (row >> 5))


def pack_tables(angles):
    wide = jnp.pad(jnp.stack([jnp.cos(angles), jnp.sin(angles)]), ((0, 0), (0, KP - K), (0, 0)))
    return wide.transpose(2, 0, 1).reshape(256, 2 * KP).astype(bf16)


def pack_mats(translate):
    wide = jnp.pad(translate, ((0, 0), (0, 0), (0, KP - K), (0, KP - K)))
    return wide.transpose(1, 3, 0, 2).reshape(2 * KP, 2 * KP)


def shards(weights, translate, angles, box_ids):
    packed = pack_columns(weights, box_ids).reshape(256, 8, 128)
    got = lax.all_to_all(packed, OUT, 0, 0, tiled=True).reshape(2048, 128)
    side = jnp.stack([lax.axis_index("zh"), lax.axis_index("core")])
    tables, mats = pack_tables(angles), pack_mats(translate)
    enter, order = row_orders()
    keep, send, labels = open_levels(side, got, tables, mats, enter)
    far = lax.ppermute(send, "core", [(0, 1), (1, 0)])
    out = close_levels(side, keep, far, labels, tables, mats, order)
    back = lax.all_to_all(out.reshape(128, 7, 2, 128), BACK, 0, 0, tiled=True)
    return unpack_columns(back.reshape(1792, 128))


def solution(mesh):
    grid = Mesh(mesh.devices.reshape(4, 2, 4, 2, 8), AXES)
    columns = P(None, None, AXES)
    return jax.shard_map(
        shards,
        mesh=grid,
        in_specs=(columns, P(), P(), P(None, AXES)),
        out_specs=columns,
        check_vma=False,
    )
```

```python
import jax
import jax.numpy as jnp
from jax import lax
from jax.experimental import pallas as pl
from jax.experimental.pallas import tpu as pltpu
from jax.sharding import Mesh, PartitionSpec as P

K = 216
KP = 256
HALF = 256
ROWS = 256
LEVELS = 9
AXES = ("y", "zh", "x", "core", "zl")
OUT = ("zh", "zl", "y", "x")
BACK = ("zl", "y", "x")
ID_LANE = K + 16
TAIL = K - 128
ROOM = 128 - TAIL
AHEAD = (4, 5, 6, 7, 8)
BITS = {1: 5, 2: 6, 4: 3, 5: 4, 6: 5, 7: 6, 8: 7}
f32 = jnp.float32
bf16 = jnp.bfloat16


def dot(a, b):
    return jnp.dot(a, b, preferred_element_type=f32)


def look_up(ids, tables):
    boxes = lax.broadcasted_iota(jnp.int32, (ids.shape[0], KP), 1).astype(f32)
    return dot(jnp.where(ids == boxes, 1.0, 0.0).astype(bf16), tables)


def turn(picked, state):
    cosines, sines = picked[:, :KP], picked[:, KP:]
    re, im = state[:, :KP], state[:, KP:]
    return cosines * re - sines * im, sines * re + cosines * im


def split(plane, block):
    parts = plane.reshape(plane.shape[0] // (2 * block), 2, block, KP)
    half = plane.shape[0] // 2
    return jnp.concatenate(
        [parts[:, 0].reshape(half, KP), parts[:, 1].reshape(half, KP)], axis=1
    ).astype(bf16)


def level(state, picked, mats, bit):
    block = 1 << bit
    stacked = []
    for half in range(2):
        re, im = turn(picked[half], state[half])
        stacked += [split(re, block), split(im, block)]
    mixed = dot(jnp.concatenate(stacked, axis=0), mats)
    quarter = ROWS // 2
    fresh = []
    for target in range(2):
        planes = []
        for plane in range(2):
            pieces = [
                mixed[
                    (2 * half + plane) * quarter : (2 * half + plane + 1) * quarter,
                    target * KP : (target + 1) * KP,
                ].reshape(quarter // block, 1, block, KP)
                for half in range(2)
            ]
            planes.append(jnp.concatenate(pieces, axis=1).reshape(ROWS, KP))
        fresh.append(jnp.concatenate(planes, axis=1).astype(bf16).astype(f32))
    return fresh


def ids(labels, number):
    first = TAIL + number - 1
    return [labels[:, first + 8 * half : first + 8 * half + 1] for half in range(2)]


def both(labels, number, tables):
    return [look_up(tags, tables) for tags in ids(labels, number)]


def round_to(values):
    return values.astype(bf16).astype(f32)


def opening(side_ref, got_ref, tab_ref, mat_ref, order_ref, keep_ref, send_ref, label_ref, rows_ref):
    tables = tab_ref[...]
    mats = mat_ref[...]
    quarter = ROWS // 2
    rows_ref[...] = got_ref[...].astype(f32)
    stacked, labels = [], []
    for kept in range(2):
        got = jnp.concatenate(
            [rows_ref[pl.ds(4 * kept + part, ROWS, stride=8), :] for part in range(4)], axis=1
        )
        got = dot(order_ref[...], got.astype(bf16))
        re, im = turn(look_up(got[:, ID_LANE : ID_LANE + 1], tables), got)
        stacked += [split(re, quarter), split(im, quarter)]
        tags = got[:, 128:256]
        labels.append(jnp.where(side_ref[0] == 0, tags[:quarter], tags[quarter:]))
    labels = jnp.concatenate(labels, axis=0)
    mixed = dot(jnp.concatenate(stacked, axis=0), mats)
    state = []
    for target in range(2):
        lanes = slice(target * KP, (target + 1) * KP)
        blocks = [mixed[n * quarter : (n + 1) * quarter, lanes] for n in range(4)]
        state.append(
            round_to(
                jnp.concatenate(
                    [
                        jnp.concatenate(blocks[:2], axis=1),
                        jnp.concatenate(blocks[2:], axis=1),
                    ],
                    axis=0,
                )
            )
        )
    for number in (1, 2):
        state = level(state, both(labels, number, tables), mats, BITS[number])
    picked = both(labels, 3, tables)
    turned = [
        jnp.concatenate(turn(picked[half], state[half]), axis=1).astype(bf16)
        for half in range(2)
    ]
    low = side_ref[1] == 0
    keep_ref[...] = jnp.where(low, turned[0], turned[1])
    send_ref[...] = jnp.where(low, turned[1], turned[0])
    label_ref[...] = labels.astype(bf16)


def tail_lanes(part):
    lane = lax.broadcasted_iota(jnp.int32, (ROWS // 2, 128), 1)
    return (lane >= part * ROOM) & (lane < (part + 1) * ROOM)


def lookup(label_ref, tab_ref, order_ref, out_ref):
    tables = tab_ref[...]
    early = label_ref[...].astype(f32)
    late = dot(order_ref[...], label_ref[...])
    for number in AHEAD:
        picked = both(early if number < 6 else late, number, tables)
        for half in range(2):
            out_ref[2 * (number - AHEAD[0]) + half] = picked[half].astype(bf16)


def closing(side_ref, keep_ref, got_ref, label_ref, picked_ref, tab_ref, mat_ref, order_ref, out_ref, rows_ref):
    tables = tab_ref[...]
    mats = mat_ref[...]
    order = order_ref[...]
    late = dot(order, label_ref[...])

    def angles_of(number):
        if number not in AHEAD:
            return both(late, number, tables)
        first = 2 * (number - AHEAD[0])
        return [picked_ref[first + half].astype(f32) for half in range(2)]

    flipped = jnp.concatenate([mats[KP:], mats[:KP]], axis=0)
    mixed = dot(
        jnp.concatenate(
            [
                jnp.concatenate([keep_ref[:, :KP], got_ref[:, :KP]], axis=1),
                jnp.concatenate([keep_ref[:, KP:], got_ref[:, KP:]], axis=1),
            ],
            axis=0,
        ),
        jnp.where(side_ref[1] == 0, mats, flipped),
    )
    state = [
        round_to(
            jnp.concatenate(
                [
                    mixed[:ROWS, target * KP : (target + 1) * KP],
                    mixed[ROWS:, target * KP : (target + 1) * KP],
                ],
                axis=1,
            )
        )
        for target in range(2)
    ]
    for number in (4, 5):
        state = level(state, angles_of(number), mats, BITS[number])
    state = [dot(order, half.astype(bf16)) for half in state]
    for number in (6, 7, 8):
        state = level(state, angles_of(number), mats, BITS[number])
    quarter = ROWS // 2
    tails = []
    done = [half.reshape(8, 2, 16, 2 * KP) for half in state]
    for kept in range(2):
        for half in range(2):
            column = done[half][:, kept].reshape(quarter, 2 * KP)
            for plane in range(2):
                rows_ref[pl.ds(4 * kept + 2 * half + plane, quarter, stride=14), :] = column[
                    :, plane * KP : plane * KP + 128
                ]
                tails.append(column[:, plane * KP + 128 : (plane + 1) * KP])
    for row in range(6):
        part = row % 3
        guest = jnp.where(tail_lanes(part), tails[6 + row // 3], 0.0)
        guest = pltpu.roll(guest, TAIL - part * ROOM, 1)
        rows_ref[pl.ds(8 + row, quarter, stride=14), :] = tails[row] + guest
    out_ref[...] = rows_ref[...].astype(bf16)


VMEM = pl.BlockSpec(memory_space=pltpu.VMEM)
SMEM = pl.BlockSpec(memory_space=pltpu.SMEM)
GRANT = pltpu.CompilerParams(vmem_limit_bytes=20 * 2**20)


def open_levels(side, got, tables, mats, order):
    half = jax.ShapeDtypeStruct((ROWS, 2 * KP), bf16)
    return pl.pallas_call(
        opening,
        out_shape=(half, half, jax.ShapeDtypeStruct((ROWS, 128), bf16)),
        in_specs=[SMEM] + [VMEM] * 4,
        out_specs=(VMEM, VMEM, VMEM),
        scratch_shapes=[pltpu.VMEM((2048, 128), f32)],
        compiler_params=GRANT,
        name="opening",
    )(side, got, tables, mats, order)


def look_ahead(labels, tables, order):
    count = 2 * len(AHEAD)
    return pl.pallas_call(
        lookup,
        out_shape=jax.ShapeDtypeStruct((count, ROWS, 2 * KP), bf16),
        in_specs=[VMEM] * 3,
        out_specs=VMEM,
        compiler_params=GRANT,
        cost_estimate=pl.CostEstimate(
            flops=2 * count * ROWS * ROWS * 2 * KP,
            bytes_accessed=2 * count * ROWS * 2 * KP,
            transcendentals=0,
        ),
        name="lookup",
    )(labels, tables, order)


def close_levels(side, keep, got, labels, picked, tables, mats, order):
    return pl.pallas_call(
        closing,
        out_shape=jax.ShapeDtypeStruct((1792, 128), bf16),
        in_specs=[SMEM] + [VMEM] * 7,
        out_specs=VMEM,
        scratch_shapes=[pltpu.VMEM((1792, 128), f32)],
        compiler_params=GRANT,
        name="closing",
    )(side, keep, got, labels, picked, tables, mats, order)


def across(a, b):
    return lax.dot_general(a, b, (((1,), (1,)), ((), ())), preferred_element_type=f32)


def same_lane():
    here = lax.broadcasted_iota(jnp.int32, (128, 128), 0)
    there = lax.broadcasted_iota(jnp.int32, (128, 128), 1)
    return jnp.where(here == there, 1.0, 0.0).astype(bf16)


def pack(weights_ref, ids_ref, all_ids_ref, out_ref, rows_ref):
    own = ids_ref[...].astype(f32)
    tags = all_ids_ref[...].astype(f32)
    same = same_lane()
    for kept in range(2):
        lanes = slice(kept * 128, (kept + 1) * 128)
        labels = jnp.concatenate(
            [
                tags[1:, lanes],
                tags[1:, ROWS + kept * 128 : ROWS + (kept + 1) * 128],
                jnp.broadcast_to(own[:1, lanes], (KP - K - 16, 128)),
            ],
            axis=0,
        )
        first = jnp.concatenate([weights_ref[0, :, lanes].astype(f32), labels], axis=0)
        first = across(same, first.astype(bf16))
        second = across(same, weights_ref[1, :, lanes])
        pieces = [
            first[:, :128],
            first[:, 128:],
            second[:, :128],
            jnp.concatenate([second[:, 128:], jnp.zeros((128, KP - K), f32)], axis=1),
        ]
        for part, piece in enumerate(pieces):
            rows_ref[pl.ds(4 * kept + part, 128, stride=8), :] = piece
    out_ref[...] = rows_ref[...].astype(bf16)


def pack_columns(weights, box_ids):
    return pl.pallas_call(
        pack,
        grid=(2,),
        out_shape=jax.ShapeDtypeStruct((2048, 128), bf16),
        in_specs=[
            pl.BlockSpec((2, K, ROWS), lambda half: (0, 0, half)),
            pl.BlockSpec((LEVELS, ROWS), lambda half: (0, half)),
            pl.BlockSpec((LEVELS, 2 * ROWS), lambda half: (0, 0)),
        ],
        out_specs=pl.BlockSpec((1024, 128), lambda half: (half, 0)),
        scratch_shapes=[pltpu.VMEM((1024, 128), f32)],
        name="pack",
    )(weights, box_ids, box_ids)


def unpack(back_ref, out_ref, rows_ref):
    rows_ref[...] = back_ref[...].astype(f32)
    same = same_lane()
    count = ROWS // 2
    shared = [rows_ref[pl.ds(8 + row, count, stride=14), :] for row in range(6)]
    tails = list(shared)
    for group in range(2):
        guest = jnp.zeros((count, 128), f32)
        for part in range(3):
            moved = pltpu.roll(shared[3 * group + part], 128 - TAIL + part * ROOM, 1)
            guest = jnp.where(tail_lanes(part), moved, guest)
        tails.append(guest)
    for kept in range(2):
        for half in range(2):
            for plane in range(2):
                number = 4 * kept + 2 * half + plane
                head = rows_ref[pl.ds(number, count, stride=14), :]
                block = jnp.concatenate(
                    [
                        across(same, head.astype(bf16)),
                        across(same, tails[number].astype(bf16))[:TAIL],
                    ],
                    axis=0,
                )
                start = half * ROWS + kept * 128
                out_ref[plane, :, start : start + 128] = block.astype(bf16)


def unpack_columns(back):
    return pl.pallas_call(
        unpack,
        out_shape=jax.ShapeDtypeStruct((2, K, 512), bf16),
        in_specs=[VMEM],
        out_specs=VMEM,
        scratch_shapes=[pltpu.VMEM((1792, 128), f32)],
        compiler_params=GRANT,
        name="unpack",
    )(back)


def one_hot(source):
    return (source[:, None] == jnp.arange(ROWS)[None, :]).astype(bf16)


def row_orders():
    row = jnp.arange(ROWS)
    enter = one_hot((row & 128) + (row & 7) * 16 + ((row >> 3) & 15))
    return enter, one_hot((row & 31) * 8 + (row >> 5))


def pack_tables(angles):
    wide = jnp.pad(jnp.stack([jnp.cos(angles), jnp.sin(angles)]), ((0, 0), (0, KP - K), (0, 0)))
    return wide.transpose(2, 0, 1).reshape(256, 2 * KP).astype(bf16)


def pack_mats(translate):
    wide = jnp.pad(translate, ((0, 0), (0, 0), (0, KP - K), (0, KP - K)))
    return wide.transpose(1, 3, 0, 2).reshape(2 * KP, 2 * KP)


def shards(weights, translate, angles, box_ids):
    packed = pack_columns(weights, box_ids).reshape(256, 8, 128)
    got = lax.all_to_all(packed, OUT, 0, 0, tiled=True).reshape(2048, 128)
    side = jnp.stack([lax.axis_index("zh"), lax.axis_index("core")])
    tables, mats = pack_tables(angles), pack_mats(translate)
    enter, order = row_orders()
    keep, send, labels = open_levels(side, got, tables, mats, enter)
    far = lax.ppermute(send, "core", [(0, 1), (1, 0)])
    picked = look_ahead(labels, tables, order)
    out = close_levels(side, keep, far, labels, picked, tables, mats, order)
    back = lax.all_to_all(out.reshape(128, 7, 2, 128), BACK, 0, 0, tiled=True)
    return unpack_columns(back.reshape(1792, 128))


def solution(mesh):
    grid = Mesh(mesh.devices.reshape(4, 2, 4, 2, 8), AXES)
    columns = P(None, None, AXES)
    return jax.shard_map(
        shards,
        mesh=grid,
        in_specs=(columns, P(), P(), P(None, AXES)),
        out_specs=columns,
        check_vma=False,
    )
```

```python
import jax
import jax.numpy as jnp
from jax import lax
from jax.experimental import pallas as pl
from jax.experimental.pallas import tpu as pltpu
from jax.sharding import Mesh, PartitionSpec as P

K = 216
KP = 256
HALF = 256
ROWS = 256
LEVELS = 9
AXES = ("y", "zh", "x", "core", "zl")
OUT = ("zh", "zl", "y", "x")
BACK = ("zl", "y", "x")
ID_LANE = K + 16
TAIL = K - 128
ROOM = 128 - TAIL
AHEAD = (4, 5, 6, 7, 8)
BITS = {1: 5, 2: 6, 4: 3, 5: 4, 6: 5, 7: 6, 8: 7}
f32 = jnp.float32
bf16 = jnp.bfloat16


def dot(a, b):
    return jnp.dot(a, b, preferred_element_type=f32)


def look_up(ids, tables):
    boxes = lax.broadcasted_iota(jnp.int32, (ids.shape[0], KP), 1).astype(f32)
    return dot(jnp.where(ids == boxes, 1.0, 0.0).astype(bf16), tables)


def turn(picked, state):
    cosines, sines = picked[:, :KP], picked[:, KP:]
    re, im = state[:, :KP], state[:, KP:]
    return cosines * re - sines * im, sines * re + cosines * im


def split(plane, block):
    parts = plane.reshape(plane.shape[0] // (2 * block), 2, block, KP)
    half = plane.shape[0] // 2
    return jnp.concatenate(
        [parts[:, 0].reshape(half, KP), parts[:, 1].reshape(half, KP)], axis=1
    ).astype(bf16)


def level(state, picked, mats, bit):
    block = 1 << bit
    stacked = []
    for half in range(2):
        re, im = turn(picked[half], state[half])
        stacked += [split(re, block), split(im, block)]
    mixed = dot(jnp.concatenate(stacked, axis=0), mats)
    quarter = ROWS // 2
    fresh = []
    for target in range(2):
        planes = []
        for plane in range(2):
            pieces = [
                mixed[
                    (2 * half + plane) * quarter : (2 * half + plane + 1) * quarter,
                    target * KP : (target + 1) * KP,
                ].reshape(quarter // block, 1, block, KP)
                for half in range(2)
            ]
            planes.append(jnp.concatenate(pieces, axis=1).reshape(ROWS, KP))
        fresh.append(jnp.concatenate(planes, axis=1))
    return fresh


def ids(labels, number):
    first = TAIL + number - 1
    return [labels[:, first + 8 * half : first + 8 * half + 1] for half in range(2)]


def both(labels, number, tables):
    return [look_up(tags, tables) for tags in ids(labels, number)]


def opening(side_ref, got_ref, tab_ref, mat_ref, order_ref, keep_ref, send_ref, label_ref, rows_ref):
    tables = tab_ref[...]
    mats = mat_ref[...]
    quarter = ROWS // 2
    rows_ref[...] = got_ref[...].astype(f32)
    stacked, labels = [], []
    for kept in range(2):
        got = jnp.concatenate(
            [rows_ref[pl.ds(4 * kept + part, ROWS, stride=8), :] for part in range(4)], axis=1
        )
        got = dot(order_ref[...], got.astype(bf16))
        re, im = turn(look_up(got[:, ID_LANE : ID_LANE + 1], tables), got)
        stacked += [split(re, quarter), split(im, quarter)]
        tags = got[:, 128:256]
        labels.append(jnp.where(side_ref[0] == 0, tags[:quarter], tags[quarter:]))
    labels = jnp.concatenate(labels, axis=0)
    mixed = dot(jnp.concatenate(stacked, axis=0), mats)
    state = []
    for target in range(2):
        lanes = slice(target * KP, (target + 1) * KP)
        blocks = [mixed[n * quarter : (n + 1) * quarter, lanes] for n in range(4)]
        state.append(
            jnp.concatenate(
                [
                    jnp.concatenate(blocks[:2], axis=1),
                    jnp.concatenate(blocks[2:], axis=1),
                ],
                axis=0,
            )
        )
    for number in (1, 2):
        state = level(state, both(labels, number, tables), mats, BITS[number])
    picked = both(labels, 3, tables)
    turned = [
        jnp.concatenate(turn(picked[half], state[half]), axis=1).astype(bf16)
        for half in range(2)
    ]
    low = side_ref[1] == 0
    keep_ref[...] = jnp.where(low, turned[0], turned[1])
    send_ref[...] = jnp.where(low, turned[1], turned[0])
    label_ref[...] = labels.astype(bf16)


def tail_lanes(part):
    lane = lax.broadcasted_iota(jnp.int32, (ROWS // 2, 128), 1)
    return (lane >= part * ROOM) & (lane < (part + 1) * ROOM)


def lookup(label_ref, tab_ref, order_ref, out_ref):
    tables = tab_ref[...]
    early = label_ref[...].astype(f32)
    late = dot(order_ref[...], label_ref[...])
    for number in AHEAD:
        picked = both(early if number < 6 else late, number, tables)
        for half in range(2):
            out_ref[2 * (number - AHEAD[0]) + half] = picked[half].astype(bf16)


def closing(side_ref, keep_ref, got_ref, label_ref, picked_ref, tab_ref, mat_ref, order_ref, out_ref, rows_ref):
    tables = tab_ref[...]
    mats = mat_ref[...]
    order = order_ref[...]
    late = dot(order, label_ref[...])

    def angles_of(number):
        if number not in AHEAD:
            return both(late, number, tables)
        first = 2 * (number - AHEAD[0])
        return [picked_ref[first + half].astype(f32) for half in range(2)]

    flipped = jnp.concatenate([mats[KP:], mats[:KP]], axis=0)
    mixed = dot(
        jnp.concatenate(
            [
                jnp.concatenate([keep_ref[:, :KP], got_ref[:, :KP]], axis=1),
                jnp.concatenate([keep_ref[:, KP:], got_ref[:, KP:]], axis=1),
            ],
            axis=0,
        ),
        jnp.where(side_ref[1] == 0, mats, flipped),
    )
    state = [
        jnp.concatenate(
            [
                mixed[:ROWS, target * KP : (target + 1) * KP],
                mixed[ROWS:, target * KP : (target + 1) * KP],
            ],
            axis=1,
        )
        for target in range(2)
    ]
    for number in (4, 5):
        state = level(state, angles_of(number), mats, BITS[number])
    state = [dot(order, half.astype(bf16)) for half in state]
    for number in (6, 7, 8):
        state = level(state, angles_of(number), mats, BITS[number])
    quarter = ROWS // 2
    tails = []
    done = [half.reshape(8, 2, 16, 2 * KP) for half in state]
    for kept in range(2):
        for half in range(2):
            column = done[half][:, kept].reshape(quarter, 2 * KP)
            for plane in range(2):
                rows_ref[pl.ds(4 * kept + 2 * half + plane, quarter, stride=14), :] = column[
                    :, plane * KP : plane * KP + 128
                ]
                tails.append(column[:, plane * KP + 128 : (plane + 1) * KP])
    for row in range(6):
        part = row % 3
        guest = jnp.where(tail_lanes(part), tails[6 + row // 3], 0.0)
        guest = pltpu.roll(guest, TAIL - part * ROOM, 1)
        rows_ref[pl.ds(8 + row, quarter, stride=14), :] = tails[row] + guest
    out_ref[...] = rows_ref[...].astype(bf16)


VMEM = pl.BlockSpec(memory_space=pltpu.VMEM)
SMEM = pl.BlockSpec(memory_space=pltpu.SMEM)
GRANT = pltpu.CompilerParams(vmem_limit_bytes=20 * 2**20)
TIGHT = pltpu.CompilerParams(
    vmem_limit_bytes=20 * 2**20
)


def open_levels(side, got, tables, mats, order):
    half = jax.ShapeDtypeStruct((ROWS, 2 * KP), bf16)
    return pl.pallas_call(
        opening,
        out_shape=(half, half, jax.ShapeDtypeStruct((ROWS, 128), bf16)),
        in_specs=[SMEM] + [VMEM] * 4,
        out_specs=(VMEM, VMEM, VMEM),
        scratch_shapes=[pltpu.VMEM((2048, 128), f32)],
        compiler_params=GRANT,
        name="opening",
    )(side, got, tables, mats, order)


def look_ahead(labels, tables, order):
    count = 2 * len(AHEAD)
    return pl.pallas_call(
        lookup,
        out_shape=jax.ShapeDtypeStruct((count, ROWS, 2 * KP), bf16),
        in_specs=[VMEM] * 3,
        out_specs=VMEM,
        compiler_params=GRANT,
        cost_estimate=pl.CostEstimate(
            flops=2 * count * ROWS * ROWS * 2 * KP,
            bytes_accessed=2 * count * ROWS * 2 * KP,
            transcendentals=0,
        ),
        name="lookup",
    )(labels, tables, order)


def close_levels(side, keep, got, labels, picked, tables, mats, order):
    return pl.pallas_call(
        closing,
        out_shape=jax.ShapeDtypeStruct((1792, 128), bf16),
        in_specs=[SMEM] + [VMEM] * 7,
        out_specs=VMEM,
        scratch_shapes=[pltpu.VMEM((1792, 128), f32)],
        compiler_params=TIGHT,
        name="closing",
    )(side, keep, got, labels, picked, tables, mats, order)


def across(a, b):
    return lax.dot_general(a, b, (((1,), (1,)), ((), ())), preferred_element_type=f32)


def same_lane():
    here = lax.broadcasted_iota(jnp.int32, (128, 128), 0)
    there = lax.broadcasted_iota(jnp.int32, (128, 128), 1)
    return jnp.where(here == there, 1.0, 0.0).astype(bf16)


def pack(weights_ref, ids_ref, all_ids_ref, out_ref, rows_ref):
    own = ids_ref[...].astype(f32)
    tags = all_ids_ref[...].astype(f32)
    same = same_lane()
    for kept in range(2):
        lanes = slice(kept * 128, (kept + 1) * 128)
        labels = jnp.concatenate(
            [
                tags[1:, lanes],
                tags[1:, ROWS + kept * 128 : ROWS + (kept + 1) * 128],
                jnp.broadcast_to(own[:1, lanes], (KP - K - 16, 128)),
            ],
            axis=0,
        )
        first = jnp.concatenate([weights_ref[0, :, lanes].astype(f32), labels], axis=0)
        first = across(same, first.astype(bf16))
        second = across(same, weights_ref[1, :, lanes])
        pieces = [
            first[:, :128],
            first[:, 128:],
            second[:, :128],
            jnp.concatenate([second[:, 128:], jnp.zeros((128, KP - K), f32)], axis=1),
        ]
        for part, piece in enumerate(pieces):
            rows_ref[pl.ds(4 * kept + part, 128, stride=8), :] = piece
    out_ref[...] = rows_ref[...].astype(bf16)


def pack_columns(weights, box_ids):
    return pl.pallas_call(
        pack,
        grid=(2,),
        out_shape=jax.ShapeDtypeStruct((2048, 128), bf16),
        in_specs=[
            pl.BlockSpec((2, K, ROWS), lambda half: (0, 0, half)),
            pl.BlockSpec((LEVELS, ROWS), lambda half: (0, half)),
            pl.BlockSpec((LEVELS, 2 * ROWS), lambda half: (0, 0)),
        ],
        out_specs=pl.BlockSpec((1024, 128), lambda half: (half, 0)),
        scratch_shapes=[pltpu.VMEM((1024, 128), f32)],
        name="pack",
    )(weights, box_ids, box_ids)


def unpack(back_ref, out_ref, rows_ref):
    rows_ref[...] = back_ref[...].astype(f32)
    same = same_lane()
    count = ROWS // 2
    shared = [rows_ref[pl.ds(8 + row, count, stride=14), :] for row in range(6)]
    tails = list(shared)
    for group in range(2):
        guest = jnp.zeros((count, 128), f32)
        for part in range(3):
            moved = pltpu.roll(shared[3 * group + part], 128 - TAIL + part * ROOM, 1)
            guest = jnp.where(tail_lanes(part), moved, guest)
        tails.append(guest)
    for kept in range(2):
        for half in range(2):
            for plane in range(2):
                number = 4 * kept + 2 * half + plane
                head = rows_ref[pl.ds(number, count, stride=14), :]
                block = jnp.concatenate(
                    [
                        across(same, head.astype(bf16)),
                        across(same, tails[number].astype(bf16))[:TAIL],
                    ],
                    axis=0,
                )
                start = half * ROWS + kept * 128
                out_ref[plane, :, start : start + 128] = block.astype(bf16)


def unpack_columns(back):
    return pl.pallas_call(
        unpack,
        out_shape=jax.ShapeDtypeStruct((2, K, 512), bf16),
        in_specs=[VMEM],
        out_specs=VMEM,
        scratch_shapes=[pltpu.VMEM((1792, 128), f32)],
        compiler_params=GRANT,
        name="unpack",
    )(back)


def one_hot(source):
    return (source[:, None] == jnp.arange(ROWS)[None, :]).astype(bf16)


def row_orders():
    row = jnp.arange(ROWS)
    enter = one_hot((row & 128) + (row & 7) * 16 + ((row >> 3) & 15))
    return enter, one_hot((row & 31) * 8 + (row >> 5))


def pack_tables(angles):
    wide = jnp.pad(jnp.stack([jnp.cos(angles), jnp.sin(angles)]), ((0, 0), (0, KP - K), (0, 0)))
    return wide.transpose(2, 0, 1).reshape(256, 2 * KP).astype(bf16)


def pack_mats(translate):
    wide = jnp.pad(translate, ((0, 0), (0, 0), (0, KP - K), (0, KP - K)))
    return wide.transpose(1, 3, 0, 2).reshape(2 * KP, 2 * KP)


def shards(weights, translate, angles, box_ids):
    packed = pack_columns(weights, box_ids).reshape(256, 8, 128)
    got = lax.all_to_all(packed, OUT, 0, 0, tiled=True).reshape(2048, 128)
    side = jnp.stack([lax.axis_index("zh"), lax.axis_index("core")])
    tables, mats = pack_tables(angles), pack_mats(translate)
    enter, order = row_orders()
    keep, send, labels = open_levels(side, got, tables, mats, enter)
    far = lax.ppermute(send, "core", [(0, 1), (1, 0)])
    picked = look_ahead(labels, tables, order)
    out = close_levels(side, keep, far, labels, picked, tables, mats, order)
    back = lax.all_to_all(out.reshape(128, 7, 2, 128), BACK, 0, 0, tiled=True)
    return unpack_columns(back.reshape(1792, 128))


def solution(mesh):
    grid = Mesh(mesh.devices.reshape(4, 2, 4, 2, 8), AXES)
    columns = P(None, None, AXES)
    return jax.shard_map(
        shards,
        mesh=grid,
        in_specs=(columns, P(), P(), P(None, AXES)),
        out_specs=columns,
        check_vma=False,
    )
```

```python
import jax
import jax.numpy as jnp
from jax import lax
from jax.experimental import pallas as pl
from jax.experimental.pallas import tpu as pltpu
from jax.sharding import Mesh, PartitionSpec as P

K = 216
KP = 256
HALF = 256
ROWS = 256
LEVELS = 9
AXES = ("y", "zh", "x", "core", "zl")
OUT = ("zh", "zl", "y", "x")
BACK = ("zl", "y", "x")
ID_LANE = K + 16
TAIL = K - 128
ROOM = 128 - TAIL
AHEAD = (4, 5, 6, 7, 8)
BITS = {1: 5, 2: 6, 4: 3, 5: 4, 6: 5, 7: 6, 8: 7}
f32 = jnp.float32
bf16 = jnp.bfloat16


def dot(a, b):
    return jnp.dot(a, b, preferred_element_type=f32)


def look_up(ids, tables):
    boxes = lax.broadcasted_iota(jnp.int32, (ids.shape[0], KP), 1).astype(f32)
    return dot(jnp.where(ids == boxes, 1.0, 0.0).astype(bf16), tables)


def turn(picked, state):
    cosines, sines = picked[:, :KP], picked[:, KP:]
    re, im = state[:, :KP], state[:, KP:]
    return cosines * re - sines * im, sines * re + cosines * im


def split(plane, block):
    parts = plane.reshape(plane.shape[0] // (2 * block), 2, block, KP)
    half = plane.shape[0] // 2
    return jnp.concatenate(
        [parts[:, 0].reshape(half, KP), parts[:, 1].reshape(half, KP)], axis=1
    ).astype(bf16)


def level(state, picked, mats, bit):
    block = 1 << bit
    stacked = []
    for half in range(2):
        re, im = turn(picked[half], state[half])
        stacked += [split(re, block), split(im, block)]
    mixed = dot(jnp.concatenate(stacked, axis=0), mats)
    quarter = ROWS // 2
    fresh = []
    for target in range(2):
        planes = []
        for plane in range(2):
            pieces = [
                mixed[
                    (2 * half + plane) * quarter : (2 * half + plane + 1) * quarter,
                    target * KP : (target + 1) * KP,
                ].reshape(quarter // block, 1, block, KP)
                for half in range(2)
            ]
            planes.append(jnp.concatenate(pieces, axis=1).reshape(ROWS, KP))
        fresh.append(jnp.concatenate(planes, axis=1))
    return fresh


def ids(labels, number):
    first = TAIL + number - 1
    return [labels[:, first + 8 * half : first + 8 * half + 1] for half in range(2)]


def both(labels, number, tables):
    return [look_up(tags, tables) for tags in ids(labels, number)]


def opening(side_ref, got_ref, tab_ref, mat_ref, order_ref, keep_ref, send_ref, label_ref, rows_ref):
    tables = tab_ref[...]
    mats = mat_ref[...]
    quarter = ROWS // 2
    rows_ref[...] = got_ref[...].astype(f32)
    stacked, labels = [], []
    for kept in range(2):
        got = jnp.concatenate(
            [rows_ref[pl.ds(4 * kept + part, ROWS, stride=8), :] for part in range(4)], axis=1
        )
        got = dot(order_ref[...], got.astype(bf16))
        re, im = turn(look_up(got[:, ID_LANE : ID_LANE + 1], tables), got)
        stacked += [split(re, quarter), split(im, quarter)]
        tags = got[:, 128:256]
        labels.append(jnp.where(side_ref[0] == 0, tags[:quarter], tags[quarter:]))
    labels = jnp.concatenate(labels, axis=0)
    mixed = dot(jnp.concatenate(stacked, axis=0), mats)
    state = []
    for target in range(2):
        lanes = slice(target * KP, (target + 1) * KP)
        blocks = [mixed[n * quarter : (n + 1) * quarter, lanes] for n in range(4)]
        state.append(
            jnp.concatenate(
                [
                    jnp.concatenate(blocks[:2], axis=1),
                    jnp.concatenate(blocks[2:], axis=1),
                ],
                axis=0,
            )
        )
    for number in (1, 2):
        state = level(state, both(labels, number, tables), mats, BITS[number])
    picked = both(labels, 3, tables)
    turned = [
        jnp.concatenate(turn(picked[half], state[half]), axis=1).astype(bf16)
        for half in range(2)
    ]
    low = side_ref[1] == 0
    keep_ref[...] = jnp.where(low, turned[0], turned[1])
    send_ref[...] = jnp.where(low, turned[1], turned[0])
    label_ref[...] = labels.astype(bf16)


def tail_lanes(part):
    lane = lax.broadcasted_iota(jnp.int32, (ROWS // 2, 128), 1)
    return (lane >= part * ROOM) & (lane < (part + 1) * ROOM)


def lookup(label_ref, tab_ref, order_ref, out_ref):
    tables = tab_ref[...]
    early = label_ref[...].astype(f32)
    late = dot(order_ref[...], label_ref[...])
    for number in AHEAD:
        picked = both(early if number < 6 else late, number, tables)
        for half in range(2):
            out_ref[2 * (number - AHEAD[0]) + half] = picked[half].astype(bf16)


def closing(side_ref, keep_ref, got_ref, label_ref, picked_ref, tab_ref, mat_ref, order_ref, out_ref, rows_ref):
    tables = tab_ref[...]
    mats = mat_ref[...]
    order = order_ref[...]
    late = dot(order, label_ref[...])

    def angles_of(number):
        if number not in AHEAD:
            return both(late, number, tables)
        first = 2 * (number - AHEAD[0])
        return [picked_ref[first + half].astype(f32) for half in range(2)]

    flipped = jnp.concatenate([mats[KP:], mats[:KP]], axis=0)
    mixed = dot(
        jnp.concatenate(
            [
                jnp.concatenate([keep_ref[:, :KP], got_ref[:, :KP]], axis=1),
                jnp.concatenate([keep_ref[:, KP:], got_ref[:, KP:]], axis=1),
            ],
            axis=0,
        ),
        jnp.where(side_ref[1] == 0, mats, flipped),
    )
    state = [
        jnp.concatenate(
            [
                mixed[:ROWS, target * KP : (target + 1) * KP],
                mixed[ROWS:, target * KP : (target + 1) * KP],
            ],
            axis=1,
        )
        for target in range(2)
    ]
    for number in (4, 5):
        state = level(state, angles_of(number), mats, BITS[number])
    state = [dot(order, half.astype(bf16)) for half in state]
    for number in (6, 7, 8):
        state = level(state, angles_of(number), mats, BITS[number])
    quarter = ROWS // 2
    tails = []
    done = [half.reshape(8, 2, 16, 2 * KP) for half in state]
    for kept in range(2):
        for half in range(2):
            column = done[half][:, kept].reshape(quarter, 2 * KP)
            for plane in range(2):
                rows_ref[pl.ds(4 * kept + 2 * half + plane, quarter, stride=14), :] = column[
                    :, plane * KP : plane * KP + 128
                ]
                tails.append(column[:, plane * KP + 128 : (plane + 1) * KP])
    for row in range(6):
        part = row % 3
        guest = jnp.where(tail_lanes(part), tails[6 + row // 3], 0.0)
        guest = pltpu.roll(guest, TAIL - part * ROOM, 1)
        rows_ref[pl.ds(8 + row, quarter, stride=14), :] = tails[row] + guest
    out_ref[...] = rows_ref[...].astype(bf16)


VMEM = pl.BlockSpec(memory_space=pltpu.VMEM)
SMEM = pl.BlockSpec(memory_space=pltpu.SMEM)
GRANT = pltpu.CompilerParams(vmem_limit_bytes=20 * 2**20)
TIGHT = pltpu.CompilerParams(
    vmem_limit_bytes=20 * 2**20
)


def open_levels(side, got, tables, mats, order):
    half = jax.ShapeDtypeStruct((ROWS, 2 * KP), bf16)
    return pl.pallas_call(
        opening,
        out_shape=(half, half, jax.ShapeDtypeStruct((ROWS, 128), bf16)),
        in_specs=[SMEM] + [VMEM] * 4,
        out_specs=(VMEM, VMEM, VMEM),
        scratch_shapes=[pltpu.VMEM((2048, 128), f32)],
        compiler_params=GRANT,
        name="opening",
    )(side, got, tables, mats, order)


def look_ahead(labels, tables, order):
    count = 2 * len(AHEAD)
    return pl.pallas_call(
        lookup,
        out_shape=jax.ShapeDtypeStruct((count, ROWS, 2 * KP), bf16),
        in_specs=[VMEM] * 3,
        out_specs=VMEM,
        compiler_params=TIGHT,
        cost_estimate=pl.CostEstimate(
            flops=2 * count * ROWS * ROWS * 2 * KP,
            bytes_accessed=2 * count * ROWS * 2 * KP,
            transcendentals=0,
        ),
        name="lookup",
    )(labels, tables, order)


def close_levels(side, keep, got, labels, picked, tables, mats, order):
    return pl.pallas_call(
        closing,
        out_shape=jax.ShapeDtypeStruct((1792, 128), bf16),
        in_specs=[SMEM] + [VMEM] * 7,
        out_specs=VMEM,
        scratch_shapes=[pltpu.VMEM((1792, 128), f32)],
        compiler_params=TIGHT,
        name="closing",
    )(side, keep, got, labels, picked, tables, mats, order)


def across(a, b):
    return lax.dot_general(a, b, (((1,), (1,)), ((), ())), preferred_element_type=f32)


def same_lane():
    here = lax.broadcasted_iota(jnp.int32, (128, 128), 0)
    there = lax.broadcasted_iota(jnp.int32, (128, 128), 1)
    return jnp.where(here == there, 1.0, 0.0).astype(bf16)


def pack(weights_ref, ids_ref, all_ids_ref, out_ref, rows_ref):
    own = ids_ref[...].astype(f32)
    tags = all_ids_ref[...].astype(f32)
    same = same_lane()
    for kept in range(2):
        lanes = slice(kept * 128, (kept + 1) * 128)
        labels = jnp.concatenate(
            [
                tags[1:, lanes],
                tags[1:, ROWS + kept * 128 : ROWS + (kept + 1) * 128],
                jnp.broadcast_to(own[:1, lanes], (KP - K - 16, 128)),
            ],
            axis=0,
        )
        first = jnp.concatenate([weights_ref[0, :, lanes].astype(f32), labels], axis=0)
        first = across(same, first.astype(bf16))
        second = across(same, weights_ref[1, :, lanes])
        pieces = [
            first[:, :128],
            first[:, 128:],
            second[:, :128],
            jnp.concatenate([second[:, 128:], jnp.zeros((128, KP - K), f32)], axis=1),
        ]
        for part, piece in enumerate(pieces):
            rows_ref[pl.ds(4 * kept + part, 128, stride=8), :] = piece
    out_ref[...] = rows_ref[...].astype(bf16)


def pack_columns(weights, box_ids):
    return pl.pallas_call(
        pack,
        grid=(2,),
        out_shape=jax.ShapeDtypeStruct((2048, 128), bf16),
        in_specs=[
            pl.BlockSpec((2, K, ROWS), lambda half: (0, 0, half)),
            pl.BlockSpec((LEVELS, ROWS), lambda half: (0, half)),
            pl.BlockSpec((LEVELS, 2 * ROWS), lambda half: (0, 0)),
        ],
        out_specs=pl.BlockSpec((1024, 128), lambda half: (half, 0)),
        scratch_shapes=[pltpu.VMEM((1024, 128), f32)],
        compiler_params=pltpu.CompilerParams(),
        name="pack",
    )(weights, box_ids, box_ids)


def unpack(back_ref, out_ref, rows_ref):
    rows_ref[...] = back_ref[...].astype(f32)
    same = same_lane()
    count = ROWS // 2
    shared = [rows_ref[pl.ds(8 + row, count, stride=14), :] for row in range(6)]
    tails = list(shared)
    for group in range(2):
        guest = jnp.zeros((count, 128), f32)
        for part in range(3):
            moved = pltpu.roll(shared[3 * group + part], 128 - TAIL + part * ROOM, 1)
            guest = jnp.where(tail_lanes(part), moved, guest)
        tails.append(guest)
    for kept in range(2):
        for half in range(2):
            for plane in range(2):
                number = 4 * kept + 2 * half + plane
                head = rows_ref[pl.ds(number, count, stride=14), :]
                block = jnp.concatenate(
                    [
                        across(same, head.astype(bf16)),
                        across(same, tails[number].astype(bf16))[:TAIL],
                    ],
                    axis=0,
                )
                start = half * ROWS + kept * 128
                out_ref[plane, :, start : start + 128] = block.astype(bf16)


def unpack_columns(back):
    return pl.pallas_call(
        unpack,
        out_shape=jax.ShapeDtypeStruct((2, K, 512), bf16),
        in_specs=[VMEM],
        out_specs=VMEM,
        scratch_shapes=[pltpu.VMEM((1792, 128), f32)],
        compiler_params=TIGHT,
        name="unpack",
    )(back)


def one_hot(source):
    return (source[:, None] == jnp.arange(ROWS)[None, :]).astype(bf16)


def row_orders():
    row = jnp.arange(ROWS)
    enter = one_hot((row & 128) + (row & 7) * 16 + ((row >> 3) & 15))
    return enter, one_hot((row & 31) * 8 + (row >> 5))


def pack_tables(angles):
    wide = jnp.pad(jnp.stack([jnp.cos(angles), jnp.sin(angles)]), ((0, 0), (0, KP - K), (0, 0)))
    return wide.transpose(2, 0, 1).reshape(256, 2 * KP).astype(bf16)


def pack_mats(translate):
    wide = jnp.pad(translate, ((0, 0), (0, 0), (0, KP - K), (0, KP - K)))
    return wide.transpose(1, 3, 0, 2).reshape(2 * KP, 2 * KP)


def shards(weights, translate, angles, box_ids):
    packed = pack_columns(weights, box_ids).reshape(256, 8, 128)
    got = lax.all_to_all(packed, OUT, 0, 0, tiled=True).reshape(2048, 128)
    side = jnp.stack([lax.axis_index("zh"), lax.axis_index("core")])
    tables, mats = pack_tables(angles), pack_mats(translate)
    enter, order = row_orders()
    keep, send, labels = open_levels(side, got, tables, mats, enter)
    far = lax.ppermute(send, "core", [(0, 1), (1, 0)])
    picked = look_ahead(labels, tables, order)
    out = close_levels(side, keep, far, labels, picked, tables, mats, order)
    back = lax.all_to_all(out.reshape(128, 7, 2, 128), BACK, 0, 0, tiled=True)
    return unpack_columns(back.reshape(1792, 128))


def solution(mesh):
    grid = Mesh(mesh.devices.reshape(4, 2, 4, 2, 8), AXES)
    columns = P(None, None, AXES)
    return jax.shard_map(
        shards,
        mesh=grid,
        in_specs=(columns, P(), P(), P(None, AXES)),
        out_specs=columns,
        check_vma=False,
    )
```
